32 devices in a mesh: ep: 8 (over z, x), tp: 4 (over y, core).
Axes of the slice: x: 2, y: 2, z: 4, core: 2. Of those that a mesh axis runs over, the one named last changes fastest.
Arguments:
- latents: float32 [2048, 2048], P('ep', 'tp'), may hold values from -6 to 6
- timesteps: int32 [3], replicated, may hold values from 50 to 650, as said below
- routes: int32 [2, 2048, 2], P(None, 'ep'), may hold values from 0 to 7, all different within a row; in each aligned block of 256 rows (0 to 255, 256 to 511, ..., all dimensions but the last counted through in order) at most 96 rows name the same one
- mod_weight: bfloat16 [2048, 3, 2048], P('ep', None, 'tp'), may hold values from -0.125 to 0.125
- router_weight: bfloat16 [2048, 8], replicated, may hold values from -0.125 to 0.125
- up_weight: bfloat16 [8, 2048, 8192], P('ep', None, 'tp'), may hold values from -0.125 to 0.125
- down_weight: bfloat16 [8, 8192, 2048], P('ep', 'tp'), may hold values from -0.0625 to 0.0625
Outputs:
- student_target: float32 [2048, 2048], P('ep', 'tp')
The draws below stay inside these ranges and needn't reach their ends.
Inputs may be any that keep to these rules, and one draw needn't show every extreme that they name: timesteps fall by the same gap of 100 to 150 from each entry to the next; the first lies between 350 and 650. `routes`: the two experts of a token differ; among the 256 tokens of one index of ep in one substep, no expert is named more than 96 times, and in every substep some expert is named exactly 96 times by some index of ep.
All inputs are finite; a program needn't handle non-finite values.
Results may differ from the reference program's by a relative error of at most 0.013.
Values may be sent and summed in bfloat16 or wider, within the bound.
A program may use at most 64 MiB of HBM per device.

```python
import math
import jax
import jax.numpy as jnp
import numpy as np
from jax import lax

D = 2048
FF = 8192
TOK_DEV = 256
SUBSTEPS = 2
EXPERTS = 8
CAP = 96
TOKENS = 2048
N_EP = 8
N_TP = 4


def draw_timesteps(key, part):
    first_key, second_key = jax.random.split(jax.random.fold_in(key, 11))
    start_value = jax.random.randint(first_key, (), 350, 651)
    gap_value = jax.random.randint(second_key, (), 100, 151)
    return jnp.stack([start_value, start_value - gap_value, start_value - 2 * gap_value]).astype(jnp.int32)


def block_levels(own_key, dims, pieces, low, top_value):
    loudness, own = 1.0, jax.random.fold_in(own_key, 6)
    for position, shards_of in pieces:
        steps = jnp.exp(jax.random.uniform(jax.random.fold_in(own, position), (shards_of,), jnp.float32, low / len(pieces), top_value / len(pieces)))
        loudness = loudness * jnp.repeat(steps, dims[position] // shards_of).reshape([-1 if axis == position else 1 for axis in range(len(dims))])
    return loudness


def routed_block(own_key, own, number, rows, count, top, reach, skew):
    ranking = jax.random.permutation(own_key, count)
    packed, ordinary = portions_of(count, rows * top, reach, skew, True), portions_of(count, rows * top, reach, skew, False)
    places = jnp.arange(count)

    def named(tallies, offset_by):
        used = int((tallies > 0).sum())
        fixed = max(1, used // 4)
        moved = fixed + (places - fixed + offset_by * (used - fixed)) % max(1, count - fixed)
        return jnp.zeros((count,), jnp.int32).at[ranking[jnp.where(places < fixed, places, moved)]].set(jnp.asarray(tallies, jnp.int32))

    tallies = jnp.where(number % 4 == 0, named(packed, number // 4), named(ordinary, number - number // 4 - 1))
    mixed = jax.random.permutation(jax.random.fold_in(own, 3), count)
    source_of, receiver = mixed[0:count // 2 * 2:2], mixed[1:count // 2 * 2:2]
    slack = jnp.minimum(tallies[source_of] - 1, reach - tallies[receiver]) // 2
    slack = jnp.where((source_of == ranking[0]) | (receiver == ranking[0]) | (tallies[receiver] == 0), 0, jnp.maximum(slack, 0))
    moved = jax.random.randint(jax.random.fold_in(own, 4), (count // 2,), 0, 1 << 20) % (slack + 1)
    tallies = tallies.at[source_of].add(-moved).at[receiver].add(moved)
    labels = jnp.searchsorted(jnp.cumsum(tallies), jnp.arange(rows * top), side="right").astype(jnp.int32)
    grid = labels.reshape(top, rows).T
    grid = grid[jax.random.permutation(jax.random.fold_in(own, 1), rows)]
    offset_by = jax.random.randint(jax.random.fold_in(own, 2), (rows, 1), 0, top)
    return jnp.take_along_axis(grid, (jnp.arange(top)[None, :] + offset_by) % top, axis=1)


def portions_of(amount, total, bound, lean, full):
    weights = [(1 << 20) // math.isqrt(rank ** lean) + 1 for rank in range(1, amount + 1)]
    largest = bound if full else min(bound, max(-(-total // amount), total * weights[0] // sum(weights)))
    least = 1 if total - largest >= amount - 1 else 0
    counts, surplus = [largest] + [least] * (amount - 1), total - largest - least * (amount - 1)
    while surplus > 0:
        movable = [i for i in range(1, amount) if counts[i] < largest] or [i for i in range(1, amount) if counts[i] < bound]
        mass, remaining = sum([weights[i] for i in movable]), surplus
        for i in movable:
            extra = min(bound - counts[i], max(1, remaining * weights[i] // mass), surplus)
            counts[i] = counts[i] + extra
            surplus = surplus - extra
    return np.array(counts)


def gaussian(key, extent, scale, bound, shards=(), kind=jnp.bfloat16):
    array = jax.random.normal(key, extent, jnp.float32) * scale
    if len(shards) > 0:
        array = block_levels(key, extent, shards, -0.22, 0.18) * array
    return jnp.clip(array, min=-bound, max=bound).astype(kind)


def setup_inputs(seed: int = 0) -> dict:
    key_of = jax.random.split(jax.random.key(seed), 8)
    latents = gaussian(key_of[0], (TOKENS, D), 1.0, 6.0, ((0, 8), (1, 4)), jnp.float32)
    timesteps = draw_timesteps(jax.random.fold_in(key_of[7], 71), 0)
    routes_keys = jax.random.split(jax.random.fold_in(key_of[2], 1), SUBSTEPS * TOKENS // TOK_DEV)
    routes_turns = jax.random.permutation(jax.random.fold_in(key_of[2], 3), SUBSTEPS * TOKENS // TOK_DEV)
    routes = jax.vmap(lambda own, number: routed_block(jax.random.fold_in(key_of[2], 2), own, number, TOK_DEV, EXPERTS, 2, CAP, 2))(routes_keys, routes_turns).reshape((SUBSTEPS, TOKENS, 2))
    mod_weight = gaussian(key_of[3], (D, 3, D), D ** -0.5, 0.125, ((0, 8), (2, 4)))
    router_weight = gaussian(key_of[4], (D, EXPERTS), D ** -0.5, 0.125)
    up_weight = gaussian(key_of[5], (EXPERTS, D, FF), D ** -0.5, 0.125, ((0, 8), (2, 4)))
    down_weight = gaussian(key_of[6], (EXPERTS, FF, D), FF ** -0.5, 0.0625, ((0, 8), (1, 4)))
    return dict(latents=latents, timesteps=timesteps, routes=routes, mod_weight=mod_weight, router_weight=router_weight, up_weight=up_weight, down_weight=down_weight)


def plan(timestep):
    angle_value = (timestep.astype(jnp.float32) / 1000.0 + 0.008) / 1.008 * (math.pi / 2)
    return (jnp.cos(angle_value), jnp.sin(angle_value))

def embedding(timesteps_pair, width):
    half_width = width // 2
    frequency = jnp.exp(-math.log(10000.0) * jnp.arange(half_width, dtype=jnp.float32) / half_width)
    phases = timesteps_pair.astype(jnp.float32)[:, None] * frequency[None, :]
    return jnp.concatenate([jnp.cos(phases), jnp.sin(phases)], axis=1)

def reference(latents, timesteps, routes, mod_weight, router_weight, up_weight, down_weight):
    condition = embedding(timesteps[:2], D).astype(jnp.bfloat16)
    modulation = jnp.dot(condition, mod_weight.reshape(D, 3 * D), preferred_element_type=jnp.float32).reshape(2, 3, D)
    group_width = FF // N_TP
    most_rows = N_EP * CAP
    expert_ids = jnp.arange(EXPERTS, dtype=jnp.int32)
    current = latents
    for sub_step in range(2):
        cos_now, sin_now = plan(timesteps[sub_step])
        cos_next, sin_next = plan(timesteps[sub_step + 1])
        row_mean = lax.optimization_barrier(jnp.sum(current, axis=1)) / D
        row_var = lax.optimization_barrier(jnp.sum(current * current, axis=1)) / D - row_mean * row_mean
        normed = (current - row_mean[:, None]) * lax.rsqrt(row_var[:, None] + 1e-06)
        shift_row = modulation[sub_step, 0]
        scale_row = modulation[sub_step, 1]
        gate_row = modulation[sub_step, 2]
        full_rows = (normed * (1.0 + scale_row) + shift_row).astype(jnp.bfloat16)
        logits = jnp.dot(full_rows, router_weight, preferred_element_type=jnp.float32)
        chosen = routes[sub_step]
        one_hot = chosen[:, :, None] == expert_ids
        picked = lax.optimization_barrier(jnp.sum(jnp.where(one_hot, logits[:, None, :], jnp.float32(0.0)), axis=2))
        gate_probs = jax.nn.sigmoid(picked)
        weights = gate_probs / lax.optimization_barrier(jnp.sum(gate_probs, axis=1, keepdims=True))
        flat_ids = chosen.reshape(-1)

        def per_expert(pairs, inputs):
            expert_index, up_matrix, down_matrix = inputs
            matches = flat_ids == expert_index
            positions = jnp.nonzero(matches, size=most_rows, fill_value=0)[0].astype(jnp.int32)
            valid = jnp.arange(most_rows, dtype=jnp.int32) < jnp.sum(matches.astype(jnp.int32))
            input_rows = full_rows[positions // 2]
            hidden = jax.nn.gelu(jnp.dot(input_rows, up_matrix, preferred_element_type=jnp.float32)).astype(jnp.bfloat16)
            total = jnp.zeros((most_rows, D), jnp.float32)
            for group in range(N_TP):
                part = jnp.dot(hidden[:, group * group_width:(group + 1) * group_width], down_matrix[group * group_width:(group + 1) * group_width], preferred_element_type=jnp.float32).astype(jnp.bfloat16)
                part = lax.optimization_barrier(part)
                total = total + part.astype(jnp.float32)
            pairs = pairs.at[positions].add(jnp.where(valid[:, None], total, jnp.float32(0.0)))
            return (pairs, None)
        pairs, _ = lax.scan(per_expert, jnp.zeros((2 * TOKENS, D), jnp.float32), (expert_ids, up_weight, down_weight))
        expert_mix = lax.optimization_barrier(jnp.sum(weights[:, :, None] * pairs.reshape(TOKENS, 2, D), axis=1))
        noise_pred = current + gate_row * expert_mix
        clean_estimate = (current - sin_now * noise_pred) / cos_now
        current = cos_next * clean_estimate + sin_next * noise_pred
    cos_first, sin_first = plan(timesteps[0])
    cos_last, sin_last = plan(timesteps[2])
    sigma_ratio = sin_last / sin_first
    return (current - sigma_ratio * latents) / (cos_last - sigma_ratio * cos_first)
```

```python
import functools
import math

import jax
import jax.numpy as jnp
from jax import lax
from jax.experimental import pallas as pl
from jax.experimental.pallas import tpu as pltpu
from jax.sharding import PartitionSpec as P

MESH = pl.DeviceIdType.MESH
BF = jnp.bfloat16
F32 = jnp.float32
GROUPS = 4


def xor_of(me, j, n):
    out, bit = 0, 1
    while bit < n:
        own = lax.rem(me // bit, 2)
        out = out + (1 - own if (j // bit) % 2 else own) * bit
        bit *= 2
    return out


def turned(rows):
    r, width = rows.shape
    if r < 128:
        rows = jnp.concatenate([rows, jnp.zeros((128 - r, width), F32)], axis=0)
    return rows.T


def process_order(n_ep):
    return list(range(n_ep))


def send_order(n_ep):
    return list(range(n_ep))


SCHEDULE = (
    "A0", "A1", "A2", "A3", "R0", "R1", "L", "W0", "W1", "F0", "A4", "R2", "G0.0", "A5", "R3", "G0.1", "G0.2",
    "A6", "R4", "G0.3", "W2", "W3", "F1", "A7", "R5", "G1.0", "R6", "G1.1", "G1.2", "R7", "G1.3", "W4", "W5",
    "F2", "S0", "S1", "G2.0", "G2.1", "G2.2", "G2.3", "W6", "W7", "F3", "S2", "S3", "M0", "M1", "G3.0",
    "G3.1", "G3.2", "G3.3", "S4", "S5", "M2", "M3", "S6", "S7", "M4", "M5", "M6", "M7",
)


def kernel(
    n_ep, n_tp,
    ts, lat_h, mod_h, rt_h, rw_h, up_h, down_h,
    out,
    up_v, down_v, lat_v, cur_v, mod_v, rt_v, rw_v,
    ma_s, ma_r, mb_s, mb_r, modv, st_s, st_r, lg_s, lg_r,
    mdl, disp_v, pick_v, gate_v, mix_v,
    out_b, xb, hid, pas, par, y_s, y_r, own, ret_s, ret_r,
    wsem, ma_ss, ma_rs, mb_ss, mb_rs, st_ss, st_rs, lg_ss, lg_rs, aa_ss, aa_rs, ay_ss, ay_rs, sb_ss, sb_rs,
    pa_ss, pa_rs, ys_ss, ys_rs, re_ss, re_rs,
):
    me_e, me_t = lax.axis_index("ep"), lax.axis_index("tp")
    core, y = lax.rem(me_t, 2), me_t // 2
    n_y = n_tp // 2
    sib = (me_e, y * 2 + 1 - core)
    rows_t, width = lat_v.shape
    model = width * n_tp
    ff = hid.shape[1]
    cap = xb.shape[3]
    nb = y_s.shape[2]
    cb = n_ep // nb
    jg, bg = n_ep // GROUPS, nb // GROUPS
    group_rows = jg * cap
    nt = min(1024, ff)
    order = process_order(n_ep)
    place = {mask: j for j, mask in enumerate(order)}

    def local(src, dst, i):
        copy = pltpu.make_async_copy(src, dst, wsem.at[i])
        copy.start()
        return copy

    lat_c = local(lat_h, lat_v, 0)
    mod_c = local(mod_h, mod_v, 1)
    rt_c = local(rt_h, rt_v, 2)
    rw_c = local(rw_h.at[:, pl.ds(pl.multiple_of(me_t * width, width), width)], rw_v, 3)
    up_c = local(up_h.at[0], up_v, 4)
    down_c = local(down_h.at[0], down_v, 5)

    def peer_m(mask):
        return (xor_of(me_e, mask, n_ep), me_t)

    def peer_e(j):
        return peer_m(order[j])

    def peer_y(dy):
        return (me_e, lax.rem(y + dy, n_y) * 2 + core)

    def peer_t(dt):
        return (me_e, lax.rem(me_t + dt, n_tp))

    barrier = pltpu.get_barrier_semaphore()
    for j in range(1, n_ep):
        pl.semaphore_signal(barrier, inc=1, device_id=peer_m(j), device_id_type=MESH)
    for dt in range(1, n_tp):
        pl.semaphore_signal(barrier, inc=1, device_id=peer_t(dt), device_id_type=MESH)

    def remote(src, dst, ss, rs, to):
        return pltpu.make_async_remote_copy(
            src_ref=src, dst_ref=dst, send_sem=ss, recv_sem=rs, device_id=to, device_id_type=MESH
        )

    once = []

    def arrived(dst, ss, rs, to):
        remote(dst, dst, ss, rs, to).wait_recv()

    half = model // 2
    mod_rows = mod_v.shape[1]
    times = [ts[i].astype(F32) for i in range(3)]
    row = lax.broadcasted_iota(jnp.int32, (8, 128), 0)
    tcol = jnp.where(row == 0, times[0], jnp.where(row == 1, times[1], times[2]))
    angle = (tcol / 1000.0 + 0.008) / 1.008 * (math.pi / 2)
    cosv, sinv = jnp.cos(angle), jnp.sin(angle)
    cos_t = [cosv[i : i + 1, 0:1] for i in range(3)]
    sin_t = [sinv[i : i + 1, 0:1] for i in range(3)]
    first = lax.rem(me_e * mod_rows, half)
    feature = (lax.broadcasted_iota(jnp.int32, (8, mod_rows), 1) + first).astype(F32)
    frequency = jnp.exp(-math.log(10000.0) * feature / half)
    row = lax.broadcasted_iota(jnp.int32, (8, mod_rows), 0)
    phase = jnp.where(row == 0, times[0], times[1]) * frequency
    condition = jnp.where(me_e * mod_rows >= half, jnp.sin(phase), jnp.cos(phase)).astype(BF)
    mod_c.wait()
    parts = [jnp.dot(condition, mod_v[c], preferred_element_type=F32) for c in range(3)]
    ma_s[...] = jnp.concatenate([parts[0][0:1], parts[1][0:1]], axis=0)
    mb_s[...] = jnp.concatenate([parts[2][0:1], parts[0][1:2], parts[1][1:2], parts[2][1:2]], axis=0)
    rt_c.wait()
    rw_c.wait()
    lat_c.wait()
    cur_v[...] = lat_v[...]
    pl.semaphore_wait(barrier, n_ep + n_tp - 2)

    def share_one(src, dst, ss, rs):
        for j in range(1, n_ep):
            copy = remote(src, dst.at[j - 1], ss.at[j - 1], rs.at[j - 1], peer_m(j))
            copy.start()
            once.append(copy)

    def summed(src, dst, ss, rs):
        total = src[...]
        for j in range(1, n_ep):
            arrived(dst.at[j - 1], ss.at[j - 1], rs.at[j - 1], peer_m(j))
            total = total + dst[j - 1]
        return total

    share_one(ma_s, ma_r, ma_ss, ma_rs)
    share_one(mb_s, mb_r, mb_ss, mb_rs)

    sent = []

    def substep(sub, carry):
        pending = []

        def send(src, dst, ss, rs, to):
            copy = remote(src, dst, ss, rs, to)
            copy.start()
            pending.append(copy)

        def share(src, dst, ss, rs):
            for dt in range(1, n_tp):
                send(src.at[sub], dst.at[sub, dt - 1], ss.at[sub, dt - 1], rs.at[sub, dt - 1], peer_t(dt))

        def shared(src, dst, ss, rs):
            total = src[sub]
            for dt in range(1, n_tp):
                arrived(dst.at[sub, dt - 1], ss.at[sub, dt - 1], rs.at[sub, dt - 1], peer_t(dt))
                total = total + dst[sub, dt - 1]
            return total

        current = cur_v[...]
        sums = jnp.sum(current, axis=1, keepdims=True)
        squares = jnp.sum(current * current, axis=1, keepdims=True)
        lane = lax.broadcasted_iota(jnp.int32, (rows_t, 128), 1)
        both = jnp.where(lane == 0, sums, jnp.where(lane == 1, squares, 0.0))
        st_s[sub] = both.T[0:8]
        share(st_s, st_r, st_ss, st_rs)

        spot = lax.broadcasted_iota(jnp.int32, (n_ep, rows_t), 0)
        experts = jnp.zeros((n_ep, rows_t), jnp.int32)
        for j in range(n_ep):
            experts = jnp.where(spot == j, xor_of(me_e, order[j], n_ep), experts)
        routes = [rt_v[sub, k : k + 1, :] for k in range(2)]
        hot = [routes[k] == experts for k in range(2)]
        either = jnp.where(hot[0], 1.0, jnp.where(hot[1], 1.0, 0.0))
        earlier = lax.broadcasted_iota(jnp.int32, (rows_t, rows_t), 0) < lax.broadcasted_iota(
            jnp.int32, (rows_t, rows_t), 1
        )
        earlier = jnp.where(earlier, 1.0, 0.0).astype(BF)
        slot = jnp.dot(either.astype(BF), earlier, preferred_element_type=F32)
        slot = jnp.where(either > 0.5, slot, -1.0)
        ranks = lax.broadcasted_iota(jnp.int32, (cap, rows_t), 0).astype(F32)
        for j in range(n_ep):
            disp_v[j] = jnp.where(slot[j : j + 1] == ranks, 1.0, 0.0).astype(BF)
        slot_t = turned(slot)
        ranks = lax.broadcasted_iota(jnp.int32, (rows_t, cap), 1).astype(F32)
        for j in range(n_ep):
            pick_v[j] = jnp.where(slot_t[:, j : j + 1] == ranks, 1.0, 0.0).astype(BF)

        @pl.when(sub == 0)
        def _():
            total = summed(ma_s, ma_r, ma_ss, ma_rs)
            modv[0, 0:2] = total

        stats = turned(shared(st_s, st_r, st_ss, st_rs))
        row_mean = stats[:, 0:1] / model
        row_var = stats[:, 1:2] / model - row_mean * row_mean
        normed = (cur_v[...] - row_mean) * lax.rsqrt(row_var + 1e-06)
        mdl[...] = (normed * (1.0 + modv[sub, 1:2]) + modv[sub, 0:1]).astype(BF)
        for mask in send_order(n_ep):
            j = place[mask]
            outgoing = jnp.dot(disp_v[j], mdl[...], preferred_element_type=F32).astype(BF)
            if mask == 0:
                xb[sub, me_t, j] = outgoing
            else:
                out_b[sub, j] = outgoing
                send(out_b.at[sub, j], xb.at[sub, me_t, j], aa_ss.at[sub, j], aa_rs.at[sub, j], peer_e(j))
        lg_s[sub] = lax.dot_general(rw_v[...], mdl[...], (((1,), (1,)), ((), ())), preferred_element_type=F32)
        share(lg_s, lg_r, lg_ss, lg_rs)
        mix_v[...] = jnp.zeros((rows_t, width), F32)

        def step_a(b):
            js = pl.ds(b * cb, cb)
            for j in range(b * cb, b * cb + cb):
                if order[j] > 0:
                    arrived(xb.at[sub, me_t, j], aa_ss.at[sub, j], aa_rs.at[sub, j], peer_e(j))
            mine = xb.at[sub, me_t, js]
            for dy in range(1, n_y):
                send(mine, mine, ay_ss.at[sub, dy, b], ay_rs.at[sub, dy, b], peer_y(dy))
            send(mine, mine, sb_ss.at[sub, 0, b], sb_rs.at[sub, 0, b], sib)

        def step_r(b):
            js = pl.ds(b * cb, cb)
            for dy in range(1, n_y):
                came = xb.at[sub, lax.rem(y - dy + n_y, n_y) * 2 + core, js]
                arrived(came, ay_ss.at[sub, dy, b], ay_rs.at[sub, dy, b], peer_y(dy))
                send(came, came, sb_ss.at[sub, dy, b], sb_rs.at[sub, dy, b], sib)

        def step_w(b):
            js = pl.ds(b * cb, cb)
            for dy in range(n_y):
                came = xb.at[sub, lax.rem(y - dy + n_y, n_y) * 2 + 1 - core, js]
                arrived(came, sb_ss.at[sub, dy, b], sb_rs.at[sub, dy, b], sib)

        def step_l():
            logits = shared(lg_s, lg_r, lg_ss, lg_rs)
            ids = lax.broadcasted_iota(jnp.int32, (n_ep, rows_t), 0)
            probs = [
                jax.nn.sigmoid(jnp.sum(jnp.where(routes[k] == ids, logits, 0.0), axis=0, keepdims=True))
                for k in range(2)
            ]
            both_p = probs[0] + probs[1]
            gates = jnp.where(hot[0], probs[0] / both_p, jnp.where(hot[1], probs[1] / both_p, 0.0))
            gate_v[...] = turned(gates)

        def first_gemm(g):
            if g == 0:

                @pl.when(sub == 0)
                def _():
                    up_c.wait()

            def body(n, carry):
                at = pl.ds(pl.multiple_of(n * nt, nt), nt)
                total = None
                for t in range(n_tp):
                    rows = xb[sub, t, pl.ds(g * jg, jg)].reshape(group_rows, width)
                    term = jnp.dot(rows, up_v[pl.ds(t * width, width), at], preferred_element_type=F32)
                    total = term if total is None else total + term
                hid[:, at] = jax.nn.gelu(total).astype(BF)
                return carry

            lax.fori_loop(0, ff // nt, body, 0)

        def slice_dot(t, store):
            sw = min(512, width)

            def body(n, carry):
                at = pl.ds(pl.multiple_of(t * width + n * sw, sw), sw)
                value = jnp.dot(hid[...], down_v[:, at], preferred_element_type=F32)
                store(pl.ds(pl.multiple_of(n * sw, sw), sw), value)
                return carry

            lax.fori_loop(0, width // sw, body, 0)

        def for_sibling(g, dy):
            target = lax.rem(y + dy, n_y)

            def keep(at, value):
                pas[sub, g, dy, :, at] = value.astype(BF)

            slice_dot(target * 2 + 1 - core, keep)
            send(pas.at[sub, g, dy], par.at[sub, g, dy], pa_ss.at[sub, g, dy], pa_rs.at[sub, g, dy], sib)

        def from_sibling(g, dy):
            arrived(par.at[sub, g, dy], pa_ss.at[sub, g, dy], pa_rs.at[sub, g, dy], sib)

        def second_gemm(g, part):
            if g == 0 and part == 0:

                @pl.when(sub == 0)
                def _():
                    down_c.wait()

            if part == 0:
                for dy in range(1, n_y):
                    for_sibling(g, dy)
            elif part == 1:
                for_sibling(g, 0)
            elif part == 2:
                for dy in range(1, n_y):
                    from_sibling(g, dy)

                    def pass_on(at, value):
                        value = (value + par[sub, g, dy, :, at].astype(F32)).astype(BF)
                        y_s[sub, dy, pl.ds(g * bg, bg), :, at] = value.reshape(bg, cb * cap, value.shape[1])

                    slice_dot(lax.rem(y + dy, n_y) * 2 + core, pass_on)
                    for b in range(g * bg, g * bg + bg):
                        send(
                            y_s.at[sub, dy, b], y_r.at[sub, dy, b], ys_ss.at[sub, dy, b], ys_rs.at[sub, dy, b],
                            peer_y(dy),
                        )
            else:

                def hold(at, value):
                    own[g, :, at] = value

                slice_dot(me_t, hold)
                from_sibling(g, 0)

        def send_back(b):
            g = b // bg
            part = pl.ds((b - g * bg) * cb * cap, cb * cap)
            total = own[g, part, :] + par[sub, g, 0, part, :].astype(F32)
            for dy in range(1, n_y):
                arrived(y_r.at[sub, dy, b], ys_ss.at[sub, dy, b], ys_rs.at[sub, dy, b], peer_y(dy))
                total = total + y_r[sub, dy, b].astype(F32)
            ret_s[sub, pl.ds(b * cb, cb)] = total.astype(BF).reshape(cb, cap, width)
            for j in range(b * cb, b * cb + cb):
                if order[j] > 0:
                    send(ret_s.at[sub, j], ret_r.at[sub, j], re_ss.at[sub, j], re_rs.at[sub, j], peer_e(j))

        def mix_in(b):
            for j in range(b * cb, b * cb + cb):
                if order[j] > 0:
                    arrived(ret_r.at[sub, j], re_ss.at[sub, j], re_rs.at[sub, j], peer_e(j))
                    came = ret_r[sub, j]
                else:
                    came = ret_s[sub, j]
                mix_v[...] += gate_v[:, j : j + 1] * jnp.dot(pick_v[j], came, preferred_element_type=F32)

        steps = dict(A=step_a, R=step_r, W=step_w, F=first_gemm, S=send_back, M=mix_in)
        for word in SCHEDULE:
            if word == "L":
                step_l()
            elif word[0] == "G":
                g, part = word[1:].split(".")
                second_gemm(int(g), int(part))
            else:
                steps[word[0]](int(word[1:]))

        @pl.when(sub == 0)
        def _():
            total = summed(mb_s, mb_r, mb_ss, mb_rs)
            modv[0, 2:3] = total[0:1]
            modv[1, 0:3] = total[1:4]

        now = cur_v[...]
        noise = now + modv[sub, 2:3] * mix_v[...]
        first_sub = sub == 0
        cos_now, sin_now, cos_next, sin_next = [
            jnp.where(first_sub, a, b)
            for a, b in (
                (cos_t[0], cos_t[1]), (sin_t[0], sin_t[1]), (cos_t[1], cos_t[2]), (sin_t[1], sin_t[2])
            )
        ]
        clean = (now - sin_now * noise) * (1.0 / cos_now)
        cur_v[...] = cos_next * clean + sin_next * noise
        sent.extend(pending)
        for copy in pending:
            copy.wait_send()
        return carry

    lax.fori_loop(0, 2, substep, 0)
    ratio = sin_t[2] / sin_t[0]
    scale = 1.0 / (cos_t[2] - ratio * cos_t[0])
    out[...] = (cur_v[...] - ratio * lat_v[...]) * scale
    for copy in once:
        copy.wait_send()


def per_device(n_ep, n_tp, latents, timesteps, routes, mod_weight, router_weight, up_weight, down_weight):
    tok_rows, width = latents.shape
    model, experts = router_weight.shape
    capacity = 3 * tok_rows // experts
    cap = -(-capacity // 16) * 16
    ff = up_weight.shape[2]
    mod_rows = mod_weight.shape[0]
    n_y = n_tp // 2
    nb = min(8, n_ep)
    cb = n_ep // nb
    group_rows = n_ep // GROUPS * cap
    vm = pltpu.VMEM
    dma = pltpu.SemaphoreType.DMA
    scratch = [
        vm((model, ff), BF),
        vm((ff, model), BF),
        vm((tok_rows, width), F32),
        vm((tok_rows, width), F32),
        vm((3, mod_rows, width), BF),
        vm((2, 2, tok_rows), jnp.int32),
        vm((experts, width), BF),
        vm((2, width), F32),
        vm((n_ep - 1, 2, width), F32),
        vm((4, width), F32),
        vm((n_ep - 1, 4, width), F32),
        vm((2, 8, width), F32),
        vm((2, 8, tok_rows), F32),
        vm((2, n_tp - 1, 8, tok_rows), F32),
        vm((2, experts, tok_rows), F32),
        vm((2, n_tp - 1, experts, tok_rows), F32),
        vm((tok_rows, width), BF),
        vm((n_ep, cap, tok_rows), BF),
        vm((n_ep, tok_rows, cap), BF),
        vm((tok_rows, 128), F32),
        vm((tok_rows, width), F32),
        vm((2, n_ep, cap, width), BF),
        vm((2, n_tp, n_ep, cap, width), BF),
        vm((group_rows, ff), BF),
        vm((2, GROUPS, n_y, group_rows, width), BF),
        vm((2, GROUPS, n_y, group_rows, width), BF),
        vm((2, n_y, nb, cb * cap, width), BF),
        vm((2, n_y, nb, cb * cap, width), BF),
        vm((GROUPS, group_rows, width), F32),
        vm((2, n_ep, cap, width), BF),
        vm((2, n_ep, cap, width), BF),
        dma((6,)),
        dma((n_ep - 1,)), dma((n_ep - 1,)),
        dma((n_ep - 1,)), dma((n_ep - 1,)),
        dma((2, n_tp - 1)), dma((2, n_tp - 1)),
        dma((2, n_tp - 1)), dma((2, n_tp - 1)),
        dma((2, n_ep)), dma((2, n_ep)),
        dma((2, n_y, nb)), dma((2, n_y, nb)),
        dma((2, n_y, nb)), dma((2, n_y, nb)),
        dma((2, GROUPS, n_y)), dma((2, GROUPS, n_y)),
        dma((2, n_y, nb)), dma((2, n_y, nb)),
        dma((2, n_ep)), dma((2, n_ep)),
    ]
    return pl.pallas_call(
        functools.partial(kernel, n_ep, n_tp),
        out_shape=jax.ShapeDtypeStruct((tok_rows, width), F32),
        in_specs=[pl.BlockSpec(memory_space=pltpu.SMEM)] + [pl.BlockSpec(memory_space=pltpu.HBM)] * 6,
        out_specs=pl.BlockSpec(memory_space=pltpu.VMEM),
        scratch_shapes=scratch,
        compiler_params=pltpu.CompilerParams(
            collective_id=0, has_side_effects=True, vmem_limit_bytes=60 * 1024 * 1024
        ),
    )(
        timesteps, latents, jnp.swapaxes(mod_weight, 0, 1), jnp.swapaxes(routes, 1, 2), router_weight.T,
        up_weight, down_weight,
    )


def solution(mesh):
    in_specs = (
        P("ep", "tp"),
        P(),
        P(None, "ep", None),
        P("ep", None, "tp"),
        P(),
        P("ep", None, "tp"),
        P("ep", "tp", None),
    )
    body = functools.partial(per_device, mesh.shape["ep"], mesh.shape["tp"])
    return jax.shard_map(body, mesh=mesh, in_specs=in_specs, out_specs=P("ep", "tp"), check_vma=False)
```

```python
import functools
import math

import jax
import jax.numpy as jnp
from jax import lax
from jax.experimental import pallas as pl
from jax.experimental.pallas import tpu as pltpu
from jax.sharding import PartitionSpec as P

MESH = pl.DeviceIdType.MESH
BF = jnp.bfloat16
F32 = jnp.float32
GROUPS = 4


def xor_of(me, j, n):
    out, bit = 0, 1
    while bit < n:
        own = lax.rem(me // bit, 2)
        out = out + (1 - own if (j // bit) % 2 else own) * bit
        bit *= 2
    return out


def turned(rows):
    r, width = rows.shape
    if r < 128:
        rows = jnp.concatenate([rows, jnp.zeros((128 - r, width), F32)], axis=0)
    return rows.T


def process_order(n_ep):
    return [4, 2, 5, 3, 6, 1] + list(range(7, n_ep)) + [0]


def send_order(n_ep):
    return [0, 1, 2, 4, 3] + list(range(5, n_ep))


SCHEDULE = (
    "X0", "X1", "A7", "A5", "A1", "R7", "A0", "R5", "L", "R1", "A3", "T", "R0", "W1", "W0", "F0.0", "A2",
    "R3", "F0.1", "A4", "R2", "G0.0", "G0.1", "A6", "G0.2", "G0.3", "W3", "W2", "F1.0", "R4", "F1.1", "R6",
    "G1.0", "G1.1", "S0", "G1.2", "S1", "G1.3", "W5", "W4", "F2.0", "F2.1", "G2.0", "G2.1", "S2", "G2.2",
    "S3", "G2.3", "W7", "W6", "F3.0", "F3.1", "G3.0", "G3.1", "S4", "G3.2", "S5", "G3.3", "M0", "M1", "M2",
    "M3", "S6", "S7", "M4", "M5", "M7", "M6",
)


def kernel(
    n_ep, n_tp,
    ts, lat_h, mod_h, rt_h, rw_h, up_h, down_h,
    out,
    up_v, down_v, lat_v, cur_v, mod_v, rt_v, rw_v,
    ma_s, ma_r, mb_s, mb_r, modv, st_s, st_r, lg_s, lg_r,
    mdl, disp_v, pick_v, gate_v, mix_v,
    out_b, xb, hid, pas, par, y_s, y_r, own, ret_s, ret_r,
    wsem, ma_ss, ma_rs, mb_ss, mb_rs, st_ss, st_rs, lg_ss, lg_rs, aa_ss, aa_rs, ay_ss, ay_rs, sb_ss, sb_rs,
    pa_ss, pa_rs, ys_ss, ys_rs, re_ss, re_rs,
):
    me_e, me_t = lax.axis_index("ep"), lax.axis_index("tp")
    core, y = lax.rem(me_t, 2), me_t // 2
    n_y = n_tp // 2
    sib = (me_e, y * 2 + 1 - core)
    rows_t, width = lat_v.shape
    model = width * n_tp
    ff = hid.shape[1]
    cap = xb.shape[3]
    nb = y_s.shape[2]
    cb = n_ep // nb
    jg, bg = n_ep // GROUPS, nb // GROUPS
    group_rows = jg * cap
    nt = ff // 2
    order = process_order(n_ep)
    place = {mask: j for j, mask in enumerate(order)}
    held = send_order(n_ep)[6:]

    def local(src, dst, i):
        copy = pltpu.make_async_copy(src, dst, wsem.at[i])
        copy.start()
        return copy

    lat_c = local(lat_h, lat_v, 0)
    mod_c = local(mod_h, mod_v, 1)
    rt_c = local(rt_h, rt_v, 2)
    rw_c = local(rw_h.at[:, pl.ds(pl.multiple_of(me_t * width, width), width)], rw_v, 3)
    up_c = local(up_h.at[0], up_v, 4)
    down_c = local(down_h.at[0], down_v, 5)

    def peer_m(mask):
        return (xor_of(me_e, mask, n_ep), me_t)

    def peer_e(j):
        return peer_m(order[j])

    def peer_y(dy):
        return (me_e, lax.rem(y + dy, n_y) * 2 + core)

    def peer_t(dt):
        return (me_e, lax.rem(me_t + dt, n_tp))

    barrier = pltpu.get_barrier_semaphore()
    for j in range(1, n_ep):
        pl.semaphore_signal(barrier, inc=1, device_id=peer_m(j), device_id_type=MESH)
    for dt in range(1, n_tp):
        pl.semaphore_signal(barrier, inc=1, device_id=peer_t(dt), device_id_type=MESH)

    def remote(src, dst, ss, rs, to):
        return pltpu.make_async_remote_copy(
            src_ref=src, dst_ref=dst, send_sem=ss, recv_sem=rs, device_id=to, device_id_type=MESH
        )

    once = []

    def arrived(dst, ss, rs, to):
        remote(dst, dst, ss, rs, to).wait_recv()

    half = model // 2
    mod_rows = mod_v.shape[1]
    times = [ts[i].astype(F32) for i in range(3)]
    row = lax.broadcasted_iota(jnp.int32, (8, 128), 0)
    tcol = jnp.where(row == 0, times[0], jnp.where(row == 1, times[1], times[2]))
    angle = (tcol / 1000.0 + 0.008) / 1.008 * (math.pi / 2)
    cosv, sinv = jnp.cos(angle), jnp.sin(angle)
    cos_t = [cosv[i : i + 1, 0:1] for i in range(3)]
    sin_t = [sinv[i : i + 1, 0:1] for i in range(3)]
    first = lax.rem(me_e * mod_rows, half)
    feature = (lax.broadcasted_iota(jnp.int32, (8, mod_rows), 1) + first).astype(F32)
    frequency = jnp.exp(-math.log(10000.0) * feature / half)
    row = lax.broadcasted_iota(jnp.int32, (8, mod_rows), 0)
    phase = jnp.where(row == 0, times[0], times[1]) * frequency
    condition = jnp.where(me_e * mod_rows >= half, jnp.sin(phase), jnp.cos(phase)).astype(BF)
    mod_c.wait()
    parts = [jnp.dot(condition, mod_v[c], preferred_element_type=F32) for c in range(3)]
    ma_s[...] = jnp.concatenate([parts[0][0:1], parts[1][0:1]], axis=0)
    mb_s[...] = jnp.concatenate([parts[2][0:1], parts[0][1:2], parts[1][1:2], parts[2][1:2]], axis=0)
    rt_c.wait()
    rw_c.wait()
    lat_c.wait()
    cur_v[...] = lat_v[...]
    pl.semaphore_wait(barrier, n_ep + n_tp - 2)

    def share_one(src, dst, ss, rs):
        for j in range(1, n_ep):
            copy = remote(src, dst.at[j - 1], ss.at[j - 1], rs.at[j - 1], peer_m(j))
            copy.start()
            once.append(copy)

    def summed(src, dst, ss, rs):
        total = src[...]
        for j in range(1, n_ep):
            arrived(dst.at[j - 1], ss.at[j - 1], rs.at[j - 1], peer_m(j))
            total = total + dst[j - 1]
        return total

    share_one(ma_s, ma_r, ma_ss, ma_rs)
    share_one(mb_s, mb_r, mb_ss, mb_rs)

    def found(s):
        spot = lax.broadcasted_iota(jnp.int32, (n_ep, rows_t), 0)
        experts = jnp.zeros((n_ep, rows_t), jnp.int32)
        for j in range(n_ep):
            experts = jnp.where(spot == j, xor_of(me_e, order[j], n_ep), experts)
        return [rt_v[s, k : k + 1, :] == experts for k in range(2)]

    def tables(s):
        hot = found(s)
        either = jnp.where(hot[0], 1.0, jnp.where(hot[1], 1.0, 0.0))
        earlier = lax.broadcasted_iota(jnp.int32, (rows_t, rows_t), 0) < lax.broadcasted_iota(
            jnp.int32, (rows_t, rows_t), 1
        )
        earlier = jnp.where(earlier, 1.0, 0.0).astype(BF)
        slot = jnp.dot(either.astype(BF), earlier, preferred_element_type=F32)
        slot = jnp.where(either > 0.5, slot, -1.0)
        ranks = lax.broadcasted_iota(jnp.int32, (cap, rows_t), 0).astype(F32)
        for j in range(n_ep):
            disp_v[s, j] = jnp.where(slot[j : j + 1] == ranks, 1.0, 0.0).astype(BF)
        slot_t = turned(slot)
        ranks = lax.broadcasted_iota(jnp.int32, (rows_t, cap), 1).astype(F32)
        for j in range(n_ep):
            pick_v[s, j] = jnp.where(slot_t[:, j : j + 1] == ranks, 1.0, 0.0).astype(BF)


    sent = []

    def substep(sub, carry):
        pending = []

        def send(src, dst, ss, rs, to):
            copy = remote(src, dst, ss, rs, to)
            copy.start()
            pending.append(copy)

        def share(src, dst, ss, rs):
            for dt in range(1, n_tp):
                send(src.at[sub], dst.at[sub, dt - 1], ss.at[sub, dt - 1], rs.at[sub, dt - 1], peer_t(dt))

        def shared(src, dst, ss, rs):
            total = src[sub]
            for dt in range(1, n_tp):
                arrived(dst.at[sub, dt - 1], ss.at[sub, dt - 1], rs.at[sub, dt - 1], peer_t(dt))
                total = total + dst[sub, dt - 1]
            return total

        current = cur_v[...]
        sums = jnp.sum(current, axis=1, keepdims=True)
        squares = jnp.sum(current * current, axis=1, keepdims=True)
        lane = lax.broadcasted_iota(jnp.int32, (rows_t, 128), 1)
        both = jnp.where(lane == 0, sums, jnp.where(lane == 1, squares, 0.0))
        st_s[sub] = both.T[0:8]
        share(st_s, st_r, st_ss, st_rs)

        @pl.when(sub == 0)
        def _():
            tables(0)

        @pl.when(sub == 0)
        def _():
            total = summed(ma_s, ma_r, ma_ss, ma_rs)
            modv[0, 0:2] = total

        stats = turned(shared(st_s, st_r, st_ss, st_rs))
        row_mean = stats[:, 0:1] / model
        row_var = stats[:, 1:2] / model - row_mean * row_mean
        normed = (cur_v[...] - row_mean) * lax.rsqrt(row_var + 1e-06)
        mdl[...] = (normed * (1.0 + modv[sub, 1:2]) + modv[sub, 0:1]).astype(BF)
        def dispatch(j):
            send(out_b.at[sub, j], xb.at[sub, me_t, j], aa_ss.at[sub, j], aa_rs.at[sub, j], peer_e(j))

        for mask in send_order(n_ep):
            j = place[mask]
            outgoing = jnp.dot(disp_v[sub, j], mdl[...], preferred_element_type=F32).astype(BF)
            if mask == 0:
                xb[sub, me_t, j] = outgoing
            else:
                out_b[sub, j] = outgoing
                if mask not in held:
                    dispatch(j)
        lg_s[sub] = lax.dot_general(rw_v[...], mdl[...], (((1,), (1,)), ((), ())), preferred_element_type=F32)
        share(lg_s, lg_r, lg_ss, lg_rs)
        mix_v[...] = jnp.zeros((rows_t, width), F32)

        def step_x(i):
            for mask in held[i * len(held) // 2 : (i + 1) * len(held) // 2]:
                dispatch(place[mask])

        def step_a(b):
            js = pl.ds(b * cb, cb)
            for j in range(b * cb, b * cb + cb):
                if order[j] > 0:
                    arrived(xb.at[sub, me_t, j], aa_ss.at[sub, j], aa_rs.at[sub, j], peer_e(j))
            mine = xb.at[sub, me_t, js]
            for dy in range(1, n_y):
                send(mine, mine, ay_ss.at[sub, dy, b], ay_rs.at[sub, dy, b], peer_y(dy))
            send(mine, mine, sb_ss.at[sub, 0, b], sb_rs.at[sub, 0, b], sib)

        def step_r(b):
            js = pl.ds(b * cb, cb)
            for dy in range(1, n_y):
                came = xb.at[sub, lax.rem(y - dy + n_y, n_y) * 2 + core, js]
                arrived(came, ay_ss.at[sub, dy, b], ay_rs.at[sub, dy, b], peer_y(dy))
                send(came, came, sb_ss.at[sub, dy, b], sb_rs.at[sub, dy, b], sib)

        def step_w(b):
            js = pl.ds(b * cb, cb)
            for dy in range(n_y):
                came = xb.at[sub, lax.rem(y - dy + n_y, n_y) * 2 + 1 - core, js]
                arrived(came, sb_ss.at[sub, dy, b], sb_rs.at[sub, dy, b], sib)

        def step_l():
            logits = shared(lg_s, lg_r, lg_ss, lg_rs)
            ids = lax.broadcasted_iota(jnp.int32, (n_ep, rows_t), 0)
            routes = [rt_v[sub, k : k + 1, :] for k in range(2)]
            hot = found(sub)
            probs = [
                jax.nn.sigmoid(jnp.sum(jnp.where(routes[k] == ids, logits, 0.0), axis=0, keepdims=True))
                for k in range(2)
            ]
            both_p = probs[0] + probs[1]
            gates = jnp.where(hot[0], probs[0] / both_p, jnp.where(hot[1], probs[1] / both_p, 0.0))
            gate_v[...] = turned(gates)

        def first_gemm(g, part):
            if g == 0 and part == 0:

                @pl.when(sub == 0)
                def _():
                    up_c.wait()

            at = pl.ds(part * nt, nt)
            total = None
            for t in range(n_tp):
                rows = xb[sub, t, pl.ds(g * jg, jg)].reshape(group_rows, width)
                term = jnp.dot(rows, up_v[pl.ds(t * width, width), at], preferred_element_type=F32)
                total = term if total is None else total + term
            hid[:, at] = jax.nn.gelu(total).astype(BF)

        def slice_dot(t, store):
            sw = min(512, width)

            def body(n, carry):
                at = pl.ds(pl.multiple_of(t * width + n * sw, sw), sw)
                value = jnp.dot(hid[...], down_v[:, at], preferred_element_type=F32)
                store(pl.ds(pl.multiple_of(n * sw, sw), sw), value)
                return carry

            lax.fori_loop(0, width // sw, body, 0)

        def for_sibling(g, dy):
            target = lax.rem(y + dy, n_y)

            def keep(at, value):
                pas[sub, g, dy, :, at] = value.astype(BF)

            slice_dot(target * 2 + 1 - core, keep)
            send(pas.at[sub, g, dy], par.at[sub, g, dy], pa_ss.at[sub, g, dy], pa_rs.at[sub, g, dy], sib)

        def from_sibling(g, dy):
            arrived(par.at[sub, g, dy], pa_ss.at[sub, g, dy], pa_rs.at[sub, g, dy], sib)

        def second_gemm(g, part):
            if g == 0 and part == 0:

                @pl.when(sub == 0)
                def _():
                    down_c.wait()

            if part == 0:
                for dy in range(1, n_y):
                    for_sibling(g, dy)
            elif part == 1:
                for_sibling(g, 0)
            elif part == 2:
                for dy in range(1, n_y):
                    from_sibling(g, dy)

                    def pass_on(at, value):
                        value = (value + par[sub, g, dy, :, at].astype(F32)).astype(BF)
                        y_s[sub, dy, pl.ds(g * bg, bg), :, at] = value.reshape(bg, cb * cap, value.shape[1])

                    slice_dot(lax.rem(y + dy, n_y) * 2 + core, pass_on)
                    for b in range(g * bg, g * bg + bg):
                        send(
                            y_s.at[sub, dy, b], y_r.at[sub, dy, b], ys_ss.at[sub, dy, b], ys_rs.at[sub, dy, b],
                            peer_y(dy),
                        )
            else:

                def hold(at, value):
                    own[g, :, at] = value

                slice_dot(me_t, hold)
                from_sibling(g, 0)

        def send_back(b):
            g = b // bg
            part = pl.ds((b - g * bg) * cb * cap, cb * cap)
            total = own[g, part, :] + par[sub, g, 0, part, :].astype(F32)
            for dy in range(1, n_y):
                arrived(y_r.at[sub, dy, b], ys_ss.at[sub, dy, b], ys_rs.at[sub, dy, b], peer_y(dy))
                total = total + y_r[sub, dy, b].astype(F32)
            ret_s[sub, pl.ds(b * cb, cb)] = total.astype(BF).reshape(cb, cap, width)
            for j in range(b * cb, b * cb + cb):
                if order[j] > 0:
                    send(ret_s.at[sub, j], ret_r.at[sub, j], re_ss.at[sub, j], re_rs.at[sub, j], peer_e(j))

        def mix_in(b):
            for j in range(b * cb, b * cb + cb):
                if order[j] > 0:
                    arrived(ret_r.at[sub, j], re_ss.at[sub, j], re_rs.at[sub, j], peer_e(j))
                    came = ret_r[sub, j]
                else:
                    came = ret_s[sub, j]
                mix_v[...] += gate_v[:, j : j + 1] * jnp.dot(pick_v[sub, j], came, preferred_element_type=F32)

        def step_t():
            @pl.when(sub == 0)
            def _():
                tables(1)

        steps = dict(
            X=step_x, A=step_a, R=step_r, W=step_w, L=step_l, T=step_t, F=first_gemm, G=second_gemm, S=send_back, M=mix_in
        )
        for word in SCHEDULE:
            steps[word[0]](*[int(n) for n in word[1:].split(".") if n])

        @pl.when(sub == 0)
        def _():
            total = summed(mb_s, mb_r, mb_ss, mb_rs)
            modv[0, 2:3] = total[0:1]
            modv[1, 0:3] = total[1:4]

        now = cur_v[...]
        noise = now + modv[sub, 2:3] * mix_v[...]
        first_sub = sub == 0
        cos_now, sin_now, cos_next, sin_next = [
            jnp.where(first_sub, a, b)
            for a, b in (
                (cos_t[0], cos_t[1]), (sin_t[0], sin_t[1]), (cos_t[1], cos_t[2]), (sin_t[1], sin_t[2])
            )
        ]
        clean = (now - sin_now * noise) * (1.0 / cos_now)
        cur_v[...] = cos_next * clean + sin_next * noise
        sent.extend(pending)
        for copy in pending:
            copy.wait_send()
        return carry

    lax.fori_loop(0, 2, substep, 0)
    ratio = sin_t[2] / sin_t[0]
    scale = 1.0 / (cos_t[2] - ratio * cos_t[0])
    out[...] = (cur_v[...] - ratio * lat_v[...]) * scale
    for copy in once:
        copy.wait_send()


def per_device(n_ep, n_tp, latents, timesteps, routes, mod_weight, router_weight, up_weight, down_weight):
    tok_rows, width = latents.shape
    model, experts = router_weight.shape
    capacity = 3 * tok_rows // experts
    cap = -(-capacity // 16) * 16
    ff = up_weight.shape[2]
    mod_rows = mod_weight.shape[0]
    n_y = n_tp // 2
    nb = min(8, n_ep)
    cb = n_ep // nb
    group_rows = n_ep // GROUPS * cap
    vm = pltpu.VMEM
    dma = pltpu.SemaphoreType.DMA
    scratch = [
        vm((model, ff), BF),
        vm((ff, model), BF),
        vm((tok_rows, width), F32),
        vm((tok_rows, width), F32),
        vm((3, mod_rows, width), BF),
        vm((2, 2, tok_rows), jnp.int32),
        vm((experts, width), BF),
        vm((2, width), F32),
        vm((n_ep - 1, 2, width), F32),
        vm((4, width), F32),
        vm((n_ep - 1, 4, width), F32),
        vm((2, 8, width), F32),
        vm((2, 8, tok_rows), F32),
        vm((2, n_tp - 1, 8, tok_rows), F32),
        vm((2, experts, tok_rows), F32),
        vm((2, n_tp - 1, experts, tok_rows), F32),
        vm((tok_rows, width), BF),
        vm((2, n_ep, cap, tok_rows), BF),
        vm((2, n_ep, tok_rows, cap), BF),
        vm((tok_rows, 128), F32),
        vm((tok_rows, width), F32),
        vm((2, n_ep, cap, width), BF),
        vm((2, n_tp, n_ep, cap, width), BF),
        vm((group_rows, ff), BF),
        vm((2, GROUPS, n_y, group_rows, width), BF),
        vm((2, GROUPS, n_y, group_rows, width), BF),
        vm((2, n_y, nb, cb * cap, width), BF),
        vm((2, n_y, nb, cb * cap, width), BF),
        vm((GROUPS, group_rows, width), F32),
        vm((2, n_ep, cap, width), BF),
        vm((2, n_ep, cap, width), BF),
        dma((6,)),
        dma((n_ep - 1,)), dma((n_ep - 1,)),
        dma((n_ep - 1,)), dma((n_ep - 1,)),
        dma((2, n_tp - 1)), dma((2, n_tp - 1)),
        dma((2, n_tp - 1)), dma((2, n_tp - 1)),
        dma((2, n_ep)), dma((2, n_ep)),
        dma((2, n_y, nb)), dma((2, n_y, nb)),
        dma((2, n_y, nb)), dma((2, n_y, nb)),
        dma((2, GROUPS, n_y)), dma((2, GROUPS, n_y)),
        dma((2, n_y, nb)), dma((2, n_y, nb)),
        dma((2, n_ep)), dma((2, n_ep)),
    ]
    return pl.pallas_call(
        functools.partial(kernel, n_ep, n_tp),
        out_shape=jax.ShapeDtypeStruct((tok_rows, width), F32),
        in_specs=[pl.BlockSpec(memory_space=pltpu.SMEM)] + [pl.BlockSpec(memory_space=pltpu.HBM)] * 6,
        out_specs=pl.BlockSpec(memory_space=pltpu.VMEM),
        scratch_shapes=scratch,
        compiler_params=pltpu.CompilerParams(
            collective_id=0, has_side_effects=True, vmem_limit_bytes=60 * 1024 * 1024
        ),
    )(
        timesteps, latents, jnp.swapaxes(mod_weight, 0, 1), jnp.swapaxes(routes, 1, 2), router_weight.T,
        up_weight, down_weight,
    )


def solution(mesh):
    in_specs = (
        P("ep", "tp"),
        P(),
        P(None, "ep", None),
        P("ep", None, "tp"),
        P(),
        P("ep", None, "tp"),
        P("ep", "tp", None),
    )
    body = functools.partial(per_device, mesh.shape["ep"], mesh.shape["tp"])
    return jax.shard_map(body, mesh=mesh, in_specs=in_specs, out_specs=P("ep", "tp"), check_vma=False)
```

```python
import functools
import math

import jax
import jax.numpy as jnp
from jax import lax
from jax.experimental import pallas as pl
from jax.experimental.pallas import tpu as pltpu
from jax.sharding import PartitionSpec as P

MESH = pl.DeviceIdType.MESH
BF = jnp.bfloat16
F32 = jnp.float32
GROUPS = 4


def xor_of(me, j, n):
    out, bit = 0, 1
    while bit < n:
        own = lax.rem(me // bit, 2)
        out = out + (1 - own if (j // bit) % 2 else own) * bit
        bit *= 2
    return out


def turned(rows):
    r, width = rows.shape
    if r < 128:
        rows = jnp.concatenate([rows, jnp.zeros((128 - r, width), F32)], axis=0)
    return rows.T


def process_order(n_ep):
    return [4, 2, 5, 3, 6, 1] + list(range(7, n_ep)) + [0]


def send_order(n_ep):
    return [0, 1, 2, 4, 5, 3] + list(range(6, n_ep))


SCHEDULE = (
    "X0", "X1", "A7", "A5", "A1", "R7", "A0", "R5", "L", "R1", "A3", "T", "R0", "W1", "W0", "F0.0", "A2",
    "R3", "F0.1", "A4", "G0.0", "A6", "G0.1", "R2", "G0.2", "G0.3", "W3", "W2", "F1.0", "R4", "F1.1", "R6",
    "G1.0", "G1.1", "G1.2", "S0", "S1", "G1.3", "W5", "W4", "F2.0", "F2.1", "G2.0", "G2.1", "G2.2", "S2",
    "S3", "G2.3", "W7", "W6", "F3.0", "F3.1", "G3.0", "G3.1", "G3.2", "S4", "S5", "G3.3", "M0", "M1", "M2",
    "M3", "S6", "S7", "M4", "M5", "M7", "M6",
)


def kernel(
    n_ep, n_tp,
    ts, lat_h, mod_h, rt_h, rw_h, up_h, down_h,
    out,
    up_v, down_v, lat_v, cur_v, mod_v, rt_v, rw_v,
    ma_s, ma_r, mb_s, mb_r, modv, st_s, st_r, lg_s, lg_r,
    mdl, disp_v, pick_v, gate_v, mix_v,
    out_b, xb, hid, pas, par, y_s, y_r, own, ret_s, ret_r,
    wsem, ma_ss, ma_rs, mb_ss, mb_rs, st_ss, st_rs, lg_ss, lg_rs, aa_ss, aa_rs, ay_ss, ay_rs, sb_ss, sb_rs,
    pa_ss, pa_rs, ys_ss, ys_rs, re_ss, re_rs,
):
    me_e, me_t = lax.axis_index("ep"), lax.axis_index("tp")
    core, y = lax.rem(me_t, 2), me_t // 2
    n_y = n_tp // 2
    sib = (me_e, y * 2 + 1 - core)
    rows_t, width = lat_v.shape
    model = width * n_tp
    ff = hid.shape[1]
    cap = xb.shape[3]
    nb = y_s.shape[2]
    cb = n_ep // nb
    jg, bg = n_ep // GROUPS, nb // GROUPS
    group_rows = jg * cap
    nt = ff // 2
    order = process_order(n_ep)
    place = {mask: j for j, mask in enumerate(order)}
    held = send_order(n_ep)[6:]

    def local(src, dst, i):
        copy = pltpu.make_async_copy(src, dst, wsem.at[i])
        copy.start()
        return copy

    lat_c = local(lat_h, lat_v, 0)
    mod_c = local(mod_h, mod_v, 1)
    rt_c = local(rt_h, rt_v, 2)
    rw_c = local(rw_h.at[:, pl.ds(pl.multiple_of(me_t * width, width), width)], rw_v, 3)
    up_c = local(up_h.at[0], up_v, 4)
    down_c = local(down_h.at[0], down_v, 5)

    def peer_m(mask):
        return (xor_of(me_e, mask, n_ep), me_t)

    def peer_e(j):
        return peer_m(order[j])

    def peer_y(dy):
        return (me_e, lax.rem(y + dy, n_y) * 2 + core)

    def peer_t(dt):
        return (me_e, lax.rem(me_t + dt, n_tp))

    barrier = pltpu.get_barrier_semaphore()
    for j in range(1, n_ep):
        pl.semaphore_signal(barrier, inc=1, device_id=peer_m(j), device_id_type=MESH)
    for dt in range(1, n_tp):
        pl.semaphore_signal(barrier, inc=1, device_id=peer_t(dt), device_id_type=MESH)

    def remote(src, dst, ss, rs, to):
        return pltpu.make_async_remote_copy(
            src_ref=src, dst_ref=dst, send_sem=ss, recv_sem=rs, device_id=to, device_id_type=MESH
        )

    once = []

    def arrived(dst, ss, rs, to):
        remote(dst, dst, ss, rs, to).wait_recv()

    half = model // 2
    mod_rows = mod_v.shape[1]
    times = [ts[i].astype(F32) for i in range(3)]
    row = lax.broadcasted_iota(jnp.int32, (8, 128), 0)
    tcol = jnp.where(row == 0, times[0], jnp.where(row == 1, times[1], times[2]))
    angle = (tcol / 1000.0 + 0.008) / 1.008 * (math.pi / 2)
    cosv, sinv = jnp.cos(angle), jnp.sin(angle)
    cos_t = [cosv[i : i + 1, 0:1] for i in range(3)]
    sin_t = [sinv[i : i + 1, 0:1] for i in range(3)]
    first = lax.rem(me_e * mod_rows, half)
    feature = (lax.broadcasted_iota(jnp.int32, (8, mod_rows), 1) + first).astype(F32)
    frequency = jnp.exp(-math.log(10000.0) * feature / half)
    row = lax.broadcasted_iota(jnp.int32, (8, mod_rows), 0)
    phase = jnp.where(row == 0, times[0], times[1]) * frequency
    condition = jnp.where(me_e * mod_rows >= half, jnp.sin(phase), jnp.cos(phase)).astype(BF)
    mod_c.wait()
    parts = [jnp.dot(condition, mod_v[c], preferred_element_type=F32) for c in range(3)]
    ma_s[...] = jnp.concatenate([parts[0][0:1], parts[1][0:1]], axis=0)
    mb_s[...] = jnp.concatenate([parts[2][0:1], parts[0][1:2], parts[1][1:2], parts[2][1:2]], axis=0)
    rt_c.wait()
    rw_c.wait()
    lat_c.wait()
    cur_v[...] = lat_v[...]
    pl.semaphore_wait(barrier, n_ep + n_tp - 2)

    def share_one(src, dst, ss, rs):
        for j in range(1, n_ep):
            copy = remote(src, dst.at[j - 1], ss.at[j - 1], rs.at[j - 1], peer_m(j))
            copy.start()
            once.append(copy)

    def summed(src, dst, ss, rs):
        total = src[...]
        for j in range(1, n_ep):
            arrived(dst.at[j - 1], ss.at[j - 1], rs.at[j - 1], peer_m(j))
            total = total + dst[j - 1]
        return total

    share_one(ma_s, ma_r, ma_ss, ma_rs)
    share_one(mb_s, mb_r, mb_ss, mb_rs)

    def found(s):
        spot = lax.broadcasted_iota(jnp.int32, (n_ep, rows_t), 0)
        experts = jnp.zeros((n_ep, rows_t), jnp.int32)
        for j in range(n_ep):
            experts = jnp.where(spot == j, xor_of(me_e, order[j], n_ep), experts)
        return [rt_v[s, k : k + 1, :] == experts for k in range(2)]

    def tables(s):
        hot = found(s)
        either = jnp.where(hot[0], 1.0, jnp.where(hot[1], 1.0, 0.0))
        earlier = lax.broadcasted_iota(jnp.int32, (rows_t, rows_t), 0) < lax.broadcasted_iota(
            jnp.int32, (rows_t, rows_t), 1
        )
        earlier = jnp.where(earlier, 1.0, 0.0).astype(BF)
        slot = jnp.dot(either.astype(BF), earlier, preferred_element_type=F32)
        slot = jnp.where(either > 0.5, slot, -1.0)
        ranks = lax.broadcasted_iota(jnp.int32, (cap, rows_t), 0).astype(F32)
        for j in range(n_ep):
            disp_v[s, j] = jnp.where(slot[j : j + 1] == ranks, 1.0, 0.0).astype(BF)
        slot_t = turned(slot)
        ranks = lax.broadcasted_iota(jnp.int32, (rows_t, cap), 1).astype(F32)
        for j in range(n_ep):
            pick_v[s, j] = jnp.where(slot_t[:, j : j + 1] == ranks, 1.0, 0.0).astype(BF)


    sent = []

    def substep(sub, carry):
        pending = []

        def send(src, dst, ss, rs, to):
            copy = remote(src, dst, ss, rs, to)
            copy.start()
            pending.append(copy)

        def share(src, dst, ss, rs):
            for dt in range(1, n_tp):
                send(src.at[sub], dst.at[sub, dt - 1], ss.at[sub, dt - 1], rs.at[sub, dt - 1], peer_t(dt))

        def shared(src, dst, ss, rs):
            total = src[sub]
            for dt in range(1, n_tp):
                arrived(dst.at[sub, dt - 1], ss.at[sub, dt - 1], rs.at[sub, dt - 1], peer_t(dt))
                total = total + dst[sub, dt - 1]
            return total

        current = cur_v[...]
        sums = jnp.sum(current, axis=1, keepdims=True)
        squares = jnp.sum(current * current, axis=1, keepdims=True)
        lane = lax.broadcasted_iota(jnp.int32, (rows_t, 128), 1)
        both = jnp.where(lane == 0, sums, jnp.where(lane == 1, squares, 0.0))
        st_s[sub] = both.T[0:8]
        share(st_s, st_r, st_ss, st_rs)

        @pl.when(sub == 0)
        def _():
            tables(0)

        @pl.when(sub == 0)
        def _():
            total = summed(ma_s, ma_r, ma_ss, ma_rs)
            modv[0, 0:2] = total

        stats = turned(shared(st_s, st_r, st_ss, st_rs))
        row_mean = stats[:, 0:1] / model
        row_var = stats[:, 1:2] / model - row_mean * row_mean
        normed = (cur_v[...] - row_mean) * lax.rsqrt(row_var + 1e-06)
        mdl[...] = (normed * (1.0 + modv[sub, 1:2]) + modv[sub, 0:1]).astype(BF)
        def dispatch(j):
            send(out_b.at[sub, j], xb.at[sub, me_t, j], aa_ss.at[sub, j], aa_rs.at[sub, j], peer_e(j))

        for mask in send_order(n_ep):
            j = place[mask]
            outgoing = jnp.dot(disp_v[sub, j], mdl[...], preferred_element_type=F32).astype(BF)
            if mask == 0:
                xb[sub, me_t, j] = outgoing
            else:
                out_b[sub, j] = outgoing
                if mask not in held:
                    dispatch(j)
        lg_s[sub] = lax.dot_general(rw_v[...], mdl[...], (((1,), (1,)), ((), ())), preferred_element_type=F32)
        share(lg_s, lg_r, lg_ss, lg_rs)
        mix_v[...] = jnp.zeros((rows_t, width), F32)

        def step_x(i):
            for mask in held[i * len(held) // 2 : (i + 1) * len(held) // 2]:
                dispatch(place[mask])

        def step_a(b):
            js = pl.ds(b * cb, cb)
            for j in range(b * cb, b * cb + cb):
                if order[j] > 0:
                    arrived(xb.at[sub, me_t, j], aa_ss.at[sub, j], aa_rs.at[sub, j], peer_e(j))
            mine = xb.at[sub, me_t, js]
            for dy in range(1, n_y):
                send(mine, mine, ay_ss.at[sub, dy, b], ay_rs.at[sub, dy, b], peer_y(dy))
            send(mine, mine, sb_ss.at[sub, 0, b], sb_rs.at[sub, 0, b], sib)

        def step_r(b):
            js = pl.ds(b * cb, cb)
            for dy in range(1, n_y):
                came = xb.at[sub, lax.rem(y - dy + n_y, n_y) * 2 + core, js]
                arrived(came, ay_ss.at[sub, dy, b], ay_rs.at[sub, dy, b], peer_y(dy))
                send(came, came, sb_ss.at[sub, dy, b], sb_rs.at[sub, dy, b], sib)

        def step_w(b):
            js = pl.ds(b * cb, cb)
            for dy in range(n_y):
                came = xb.at[sub, lax.rem(y - dy + n_y, n_y) * 2 + 1 - core, js]
                arrived(came, sb_ss.at[sub, dy, b], sb_rs.at[sub, dy, b], sib)

        def step_l():
            logits = shared(lg_s, lg_r, lg_ss, lg_rs)
            ids = lax.broadcasted_iota(jnp.int32, (n_ep, rows_t), 0)
            routes = [rt_v[sub, k : k + 1, :] for k in range(2)]
            hot = found(sub)
            probs = [
                jax.nn.sigmoid(jnp.sum(jnp.where(routes[k] == ids, logits, 0.0), axis=0, keepdims=True))
                for k in range(2)
            ]
            both_p = probs[0] + probs[1]
            gates = jnp.where(hot[0], probs[0] / both_p, jnp.where(hot[1], probs[1] / both_p, 0.0))
            gate_v[...] = turned(gates)

        def first_gemm(g, part):
            if g == 0 and part == 0:

                @pl.when(sub == 0)
                def _():
                    up_c.wait()

            at = pl.ds(part * nt, nt)
            total = None
            for t in range(n_tp):
                rows = xb[sub, t, pl.ds(g * jg, jg)].reshape(group_rows, width)
                term = jnp.dot(rows, up_v[pl.ds(t * width, width), at], preferred_element_type=F32)
                total = term if total is None else total + term
            hid[:, at] = jax.nn.gelu(total).astype(BF)

        def slice_dot(t, store):
            sw = min(512, width)

            def body(n, carry):
                at = pl.ds(pl.multiple_of(t * width + n * sw, sw), sw)
                value = jnp.dot(hid[...], down_v[:, at], preferred_element_type=F32)
                store(pl.ds(pl.multiple_of(n * sw, sw), sw), value)
                return carry

            lax.fori_loop(0, width // sw, body, 0)

        def for_sibling(g, dy):
            target = lax.rem(y + dy, n_y)

            def keep(at, value):
                pas[sub, g, dy, :, at] = value.astype(BF)

            slice_dot(target * 2 + 1 - core, keep)
            send(pas.at[sub, g, dy], par.at[sub, g, dy], pa_ss.at[sub, g, dy], pa_rs.at[sub, g, dy], sib)

        def from_sibling(g, dy):
            arrived(par.at[sub, g, dy], pa_ss.at[sub, g, dy], pa_rs.at[sub, g, dy], sib)

        def second_gemm(g, part):
            if g == 0 and part == 0:

                @pl.when(sub == 0)
                def _():
                    down_c.wait()

            if part == 0:
                for dy in range(1, n_y):
                    for_sibling(g, dy)
            elif part == 1:
                for_sibling(g, 0)
            elif part == 2:
                for dy in range(1, n_y):
                    from_sibling(g, dy)

                    def pass_on(at, value):
                        value = (value + par[sub, g, dy, :, at].astype(F32)).astype(BF)
                        y_s[sub, dy, pl.ds(g * bg, bg), :, at] = value.reshape(bg, cb * cap, value.shape[1])

                    slice_dot(lax.rem(y + dy, n_y) * 2 + core, pass_on)
                    for b in range(g * bg, g * bg + bg):
                        send(
                            y_s.at[sub, dy, b], y_r.at[sub, dy, b], ys_ss.at[sub, dy, b], ys_rs.at[sub, dy, b],
                            peer_y(dy),
                        )
            else:

                def hold(at, value):
                    own[g, :, at] = value

                slice_dot(me_t, hold)
                from_sibling(g, 0)

        def send_back(b):
            g = b // bg
            part = pl.ds((b - g * bg) * cb * cap, cb * cap)
            total = own[g, part, :] + par[sub, g, 0, part, :].astype(F32)
            for dy in range(1, n_y):
                arrived(y_r.at[sub, dy, b], ys_ss.at[sub, dy, b], ys_rs.at[sub, dy, b], peer_y(dy))
                total = total + y_r[sub, dy, b].astype(F32)
            ret_s[sub, pl.ds(b * cb, cb)] = total.astype(BF).reshape(cb, cap, width)
            for j in range(b * cb, b * cb + cb):
                if order[j] > 0:
                    send(ret_s.at[sub, j], ret_r.at[sub, j], re_ss.at[sub, j], re_rs.at[sub, j], peer_e(j))

        def mix_in(b):
            for j in range(b * cb, b * cb + cb):
                if order[j] > 0:
                    arrived(ret_r.at[sub, j], re_ss.at[sub, j], re_rs.at[sub, j], peer_e(j))
                    came = ret_r[sub, j]
                else:
                    came = ret_s[sub, j]
                mix_v[...] += gate_v[:, j : j + 1] * jnp.dot(pick_v[sub, j], came, preferred_element_type=F32)

        def step_t():
            @pl.when(sub == 0)
            def _():
                tables(1)

        steps = dict(
            X=step_x, A=step_a, R=step_r, W=step_w, L=step_l, T=step_t, F=first_gemm, G=second_gemm, S=send_back, M=mix_in
        )
        for word in SCHEDULE:
            steps[word[0]](*[int(n) for n in word[1:].split(".") if n])

        @pl.when(sub == 0)
        def _():
            total = summed(mb_s, mb_r, mb_ss, mb_rs)
            modv[0, 2:3] = total[0:1]
            modv[1, 0:3] = total[1:4]

        now = cur_v[...]
        noise = now + modv[sub, 2:3] * mix_v[...]
        first_sub = sub == 0
        cos_now, sin_now, cos_next, sin_next = [
            jnp.where(first_sub, a, b)
            for a, b in (
                (cos_t[0], cos_t[1]), (sin_t[0], sin_t[1]), (cos_t[1], cos_t[2]), (sin_t[1], sin_t[2])
            )
        ]
        clean = (now - sin_now * noise) * (1.0 / cos_now)
        cur_v[...] = cos_next * clean + sin_next * noise
        sent.extend(pending)
        for copy in pending:
            copy.wait_send()
        return carry

    lax.fori_loop(0, 2, substep, 0)
    ratio = sin_t[2] / sin_t[0]
    scale = 1.0 / (cos_t[2] - ratio * cos_t[0])
    out[...] = (cur_v[...] - ratio * lat_v[...]) * scale
    for copy in once:
        copy.wait_send()


def per_device(n_ep, n_tp, latents, timesteps, routes, mod_weight, router_weight, up_weight, down_weight):
    tok_rows, width = latents.shape
    model, experts = router_weight.shape
    capacity = 3 * tok_rows // experts
    cap = -(-capacity // 16) * 16
    ff = up_weight.shape[2]
    mod_rows = mod_weight.shape[0]
    n_y = n_tp // 2
    nb = min(8, n_ep)
    cb = n_ep // nb
    group_rows = n_ep // GROUPS * cap
    vm = pltpu.VMEM
    dma = pltpu.SemaphoreType.DMA
    scratch = [
        vm((model, ff), BF),
        vm((ff, model), BF),
        vm((tok_rows, width), F32),
        vm((tok_rows, width), F32),
        vm((3, mod_rows, width), BF),
        vm((2, 2, tok_rows), jnp.int32),
        vm((experts, width), BF),
        vm((2, width), F32),
        vm((n_ep - 1, 2, width), F32),
        vm((4, width), F32),
        vm((n_ep - 1, 4, width), F32),
        vm((2, 8, width), F32),
        vm((2, 8, tok_rows), F32),
        vm((2, n_tp - 1, 8, tok_rows), F32),
        vm((2, experts, tok_rows), F32),
        vm((2, n_tp - 1, experts, tok_rows), F32),
        vm((tok_rows, width), BF),
        vm((2, n_ep, cap, tok_rows), BF),
        vm((2, n_ep, tok_rows, cap), BF),
        vm((tok_rows, 128), F32),
        vm((tok_rows, width), F32),
        vm((2, n_ep, cap, width), BF),
        vm((2, n_tp, n_ep, cap, width), BF),
        vm((group_rows, ff), BF),
        vm((2, GROUPS, n_y, group_rows, width), BF),
        vm((2, GROUPS, n_y, group_rows, width), BF),
        vm((2, n_y, nb, cb * cap, width), BF),
        vm((2, n_y, nb, cb * cap, width), BF),
        vm((GROUPS, group_rows, width), F32),
        vm((2, n_ep, cap, width), BF),
        vm((2, n_ep, cap, width), BF),
        dma((6,)),
        dma((n_ep - 1,)), dma((n_ep - 1,)),
        dma((n_ep - 1,)), dma((n_ep - 1,)),
        dma((2, n_tp - 1)), dma((2, n_tp - 1)),
        dma((2, n_tp - 1)), dma((2, n_tp - 1)),
        dma((2, n_ep)), dma((2, n_ep)),
        dma((2, n_y, nb)), dma((2, n_y, nb)),
        dma((2, n_y, nb)), dma((2, n_y, nb)),
        dma((2, GROUPS, n_y)), dma((2, GROUPS, n_y)),
        dma((2, n_y, nb)), dma((2, n_y, nb)),
        dma((2, n_ep)), dma((2, n_ep)),
    ]
    return pl.pallas_call(
        functools.partial(kernel, n_ep, n_tp),
        out_shape=jax.ShapeDtypeStruct((tok_rows, width), F32),
        in_specs=[pl.BlockSpec(memory_space=pltpu.SMEM)] + [pl.BlockSpec(memory_space=pltpu.HBM)] * 6,
        out_specs=pl.BlockSpec(memory_space=pltpu.VMEM),
        scratch_shapes=scratch,
        compiler_params=pltpu.CompilerParams(
            collective_id=0, has_side_effects=True, vmem_limit_bytes=60 * 1024 * 1024
        ),
    )(
        timesteps, latents, jnp.swapaxes(mod_weight, 0, 1), jnp.swapaxes(routes, 1, 2), router_weight.T,
        up_weight, down_weight,
    )


def solution(mesh):
    in_specs = (
        P("ep", "tp"),
        P(),
        P(None, "ep", None),
        P("ep", None, "tp"),
        P(),
        P("ep", None, "tp"),
        P("ep", "tp", None),
    )
    body = functools.partial(per_device, mesh.shape["ep"], mesh.shape["tp"])
    return jax.shard_map(body, mesh=mesh, in_specs=in_specs, out_specs=P("ep", "tp"), check_vma=False)
```
